32 devices in a mesh: gx: 4 (over y, x), gy: 8 (over z, core).
Axes of the slice: x: 2, y: 2, z: 4, core: 2. Of those that a mesh axis runs over, the one named last changes fastest.
Arguments:
- traces: bfloat16 [8, 16, 128, 256], P('gx', 'gy'), may hold values from -6 to 6
- aperture: int32 [8, 16, 9], P('gx', 'gy'), may hold values 0 or 1
- geometry: int32 [8, 16, 3, 128], P('gx', 'gy'), may hold values from 0 to 63, as said below
- trace_weight: bfloat16 [8, 16, 128], P('gx', 'gy'), may hold values from 0.0087890625 to 0.03515625
- class_weight: float32 [14], replicated, may hold values from 0.3 to 1.5
- traveltime: int32 [14, 256], replicated, may hold values from 0 to 1114
Outputs:
- image: float32 [64, 64, 256], P('gx', 'gy')
The draws below stay inside these ranges and needn't reach their ends.
Inputs may be any that keep to these rules, and one draw needn't show every extreme that they name: Row 0 of a trace's geometry is an inline midpoint among the 16 image columns of its block's tile, row 1 a crossline midpoint among its tile's 8 columns, row 2 an offset class below 8.
All inputs are finite; a program needn't handle non-finite values. No bound on the sum of `aperture` on one device may be relied on, other than what follows from the above.
Results may differ from the reference program's by a relative error of at most 0.0029.
Values may be sent and summed in bfloat16 or wider, within the bound.
A program may use at most 64 MiB of HBM per device.

```python
import math
import jax
import jax.numpy as jnp
from jax import lax

NS = 256
NTIME = 256
TR = 128
NH = 8
BB = 2
PX = 16
PY = 8
DSTEP = 8
NC = 14
NBX = 8
NBY = 16
NX = 64
NY = 64
N_GX = 4
N_GY = 8


def draw_geometry(key, part):
    keys = jax.random.split(jax.random.fold_in(key, 11), 3)
    block_x = jnp.arange(NBX, dtype=jnp.int32)[:, None, None] // BB
    block_y = jnp.arange(NBY, dtype=jnp.int32)[None, :, None] // BB
    inline = block_x * PX + jax.random.randint(keys[0], (NBX, NBY, TR), 0, PX)
    crossline = block_y * PY + jax.random.randint(keys[1], (NBX, NBY, TR), 0, PY)
    offset_class = jax.random.randint(keys[2], (NBX, NBY, TR), 0, NH)
    return jnp.stack([inline, crossline, offset_class], axis=2).astype(jnp.int32)


def draw_traveltime(key, part):
    level = jnp.arange(NC, dtype=jnp.int32)[:, None]
    sample = jnp.arange(NTIME, dtype=jnp.int32)[None, :]
    raw = jax.random.randint(jax.random.fold_in(key, 23), (NC, NTIME), 0, 1 << 20)
    extra = raw % (4 * level + 4)
    return (4 * sample + 3 * level + extra).astype(jnp.int32)


def touch_ends(entries, key, low, high):
    extent = entries.shape
    index_at = [jax.random.randint(jax.random.fold_in(key, axis), (), 0, extent[axis]) for axis in range(len(extent))]
    entries = entries.at[tuple(index_at)].set(low)
    longest = extent.index(max(extent))
    index_at[longest] = (index_at[longest] + 1) % extent[longest]
    return entries.at[tuple(index_at)].set(high)


def levels(stream_key, dims, pieces, least, largest):
    gain = 1.0
    for axis_at, blocks in pieces:
        steps = jax.random.uniform(jax.random.fold_in(jax.random.fold_in(stream_key, 6), axis_at), (blocks,), jnp.float32, least / len(pieces), largest / len(pieces))
        gain = gain * jnp.repeat(jnp.exp(steps), dims[axis_at] // blocks).reshape((-1,) + (1,) * (len(dims) - 1 - axis_at))
    return gain


def scatter_about(stream_key, dims, deviation, bound, cuts=(), kind=jnp.bfloat16):
    result = deviation * jax.random.normal(stream_key, dims, jnp.float32)
    if cuts:
        result = result * levels(stream_key, dims, cuts, -0.22, 0.18)
    return jnp.clip(result, -bound, bound).astype(kind)


def setup_inputs(seed: int = 0) -> dict:
    streams_of = jax.random.split(jax.random.key(seed), 7)
    return {
        "traces": scatter_about(streams_of[0], (NBX, NBY, TR, NS), 1.0, 6.0, ((0, 4), (1, 8))),
        "aperture": touch_ends((jax.random.randint(streams_of[1], (NBX, NBY, 9), 0, 3) < 2).astype(jnp.int32), jax.random.fold_in(streams_of[1], 1), 0, 1),
        "geometry": draw_geometry(jax.random.fold_in(streams_of[6], 71), 0),
        "trace_weight": jnp.clip(jnp.exp(math.log(0.03515625) - 1.3862944 * jax.random.uniform(streams_of[3], (NBX, NBY, TR), jnp.float32) ** levels(streams_of[3], (NBX, NBY, TR), ((0, 4), (1, 8)), -0.2, 0.2)), 0.0087890625, 0.03515625).astype(jnp.bfloat16),
        "class_weight": jnp.clip(jnp.exp(jax.random.uniform(streams_of[4], (NC,), jnp.float32, math.log(0.3), math.log(1.5))), 0.3, 1.5),
        "traveltime": draw_traveltime(jax.random.fold_in(streams_of[6], 71), 0),
    }


def migrate(samples_in, live_weights, geometry, tile_x, tile_y, traveltime, class_weight):
    points = jnp.arange(PX * PY, dtype=jnp.int32)
    point_x = tile_x * PX + points // PY
    point_y = tile_y * PY + points % PY
    distance = jnp.abs(point_x[:, None] - geometry[0][None, :]) + jnp.abs(point_y[:, None] - geometry[1][None, :])
    classes = geometry[2][None, :] + distance // DSTEP
    sample_ids = jnp.arange(NS, dtype=jnp.int32)[:, None]
    samples_wide = samples_in.astype(jnp.float32)

    def add_class(level, image):
        scaled = (live_weights * class_weight[level]).astype(jnp.bfloat16).astype(jnp.float32)
        amplitude = jnp.where(classes == level, scaled[None, :], jnp.float32(0.0))
        stacked = jnp.dot(amplitude, samples_wide, precision=lax.Precision.HIGHEST, preferred_element_type=jnp.float32)
        quarter = traveltime[level]
        first_sample = quarter // 4
        fraction = (quarter % 4).astype(jnp.float32) * 0.25
        interp = jnp.where(sample_ids == first_sample[None, :], 1.0 - fraction[None, :], 0.0) + jnp.where(sample_ids == first_sample[None, :] + 1, fraction[None, :], 0.0)
        return image + jnp.dot(stacked, interp.astype(jnp.float32), precision=lax.Precision.HIGHEST, preferred_element_type=jnp.float32)

    return lax.fori_loop(0, class_weight.shape[0], add_class, jnp.zeros((PX * PY, NTIME), jnp.float32))


def reference(traces, aperture, geometry, trace_weight, class_weight, traveltime):
    padded_traces = jnp.pad(traces, ((BB, BB), (BB, BB), (0, 0), (0, 0)))
    padded_aperture = jnp.pad(aperture, ((BB, BB), (BB, BB), (0, 0)))
    padded_geometry = jnp.pad(geometry, ((BB, BB), (BB, BB), (0, 0), (0, 0)))
    padded_weight = jnp.pad(trace_weight, ((BB, BB), (BB, BB), (0, 0)))
    offset = jnp.arange(3 * BB, dtype=jnp.int32) // BB - 1
    wanted = (1 - offset)[:, None] * 3 + (1 - offset)[None, :]
    choose = (jnp.arange(9, dtype=jnp.int32)[None, None, :] == wanted[:, :, None]).astype(jnp.int32)
    zero_index = jnp.int32(0)

    def one_tile(tile):
        tile_x = (tile // N_GY).astype(jnp.int32)
        tile_y = (tile % N_GY).astype(jnp.int32)
        start_x = (tile_x * BB).astype(jnp.int32)
        start_y = (tile_y * BB).astype(jnp.int32)
        near_traces = lax.dynamic_slice(padded_traces, (start_x, start_y, zero_index, zero_index), (3 * BB, 3 * BB, TR, NS))
        near_aperture = lax.dynamic_slice(padded_aperture, (start_x, start_y, zero_index), (3 * BB, 3 * BB, 9))
        near_geometry = lax.dynamic_slice(padded_geometry, (start_x, start_y, zero_index, zero_index), (3 * BB, 3 * BB, 3, TR))
        near_weight = lax.dynamic_slice(padded_weight, (start_x, start_y, zero_index), (3 * BB, 3 * BB, TR))
        live_block = jnp.sum(near_aperture * choose, axis=2)
        live = jnp.broadcast_to(live_block[:, :, None], near_weight.shape).reshape(-1)
        live_weights = near_weight.reshape(-1).astype(jnp.float32) * live.astype(jnp.float32)
        flat_geometry = jnp.moveaxis(near_geometry, 2, 0).reshape(3, -1)
        return migrate(near_traces.reshape(-1, NS), live_weights, flat_geometry, tile_x, tile_y, traveltime, class_weight)

    tiles = lax.map(one_tile, jnp.arange(N_GX * N_GY, dtype=jnp.int32))
    return tiles.reshape(N_GX, N_GY, PX, PY, NTIME).transpose(0, 2, 1, 3, 4).reshape(NX, NY, NTIME)
```

```python
import functools

import jax
import jax.numpy as jnp
from jax import lax
from jax.experimental import pallas as pl
from jax.experimental.pallas import tpu as pltpu
from jax.sharding import PartitionSpec as P

PX = 16
PY = 8
DSTEP = 8
MESH = pl.DeviceIdType.MESH
BF = jnp.bfloat16
F32 = jnp.float32

ND = (2 * PX - 1 + 2 * PY - 1) // DSTEP + 1


def classes_at(dx, dy):
    far_x = 2 * PX - 1 if dx else PX - 1
    far_y = 2 * PY - 1 if dy else PY - 1
    return (far_x + far_y) // DSTEP + 1


def kernel(
    n_x, n_y, traces, geometry, weight, traveltime, aperture, class_weight, image,
    taps, values, amplitude, diag_out, side_out, x_out, diag_in, side_in, x_in,
    send_sem, recv_sem,
):
    bx, by, tr, ns = traces.shape
    nc, nt = traveltime.shape
    nj = bx * by * tr
    cols = PX * PY
    nh = nc - ND + 1
    me_x = lax.axis_index("gx")
    me_y = lax.axis_index("gy")
    has = {
        ("gx", -1): me_x > 0,
        ("gx", 1): me_x < n_x - 1,
        ("gy", -1): me_y > 0,
        ("gy", 1): me_y < n_y - 1,
    }
    at = {"gx": me_x, "gy": me_y}
    sides = ((0, -1), (1, 1))

    barrier = pltpu.get_barrier_semaphore()
    for (axis, step), there in has.items():
        @pl.when(there)
        def _(axis=axis, step=step):
            pl.semaphore_signal(
                barrier, inc=1, device_id={axis: at[axis] + step}, device_id_type=MESH
            )

    def copy(src, dst, number, axis, step):
        return pltpu.make_async_remote_copy(
            src_ref=src, dst_ref=dst,
            send_sem=send_sem.at[number], recv_sem=recv_sem.at[number],
            device_id={axis: at[axis] + step}, device_id_type=MESH,
        )

    diag = [copy(diag_out.at[k], diag_in.at[k], k, "gy", s) for k, s in sides]
    side = [copy(side_out.at[k], side_in.at[k], 2 + k, "gy", s) for k, s in sides]
    across = [copy(x_out.at[k], x_in.at[k], 4 + k, "gx", s) for k, s in sides]

    def start(copies, axis):
        for k, s in sides:
            @pl.when(has[axis, s])
            def _(k=k):
                copies[k].start()

    def arrive(copies, axis, landed):
        for k, s in sides:
            @pl.when(has[axis, -s])
            def _(k=k):
                copies[k].wait_recv()

            @pl.when(jnp.logical_not(has[axis, -s]))
            def _(k=k):
                landed[k] = jnp.zeros(landed.shape[1:], landed.dtype)

    def sent(copies, axis):
        for k, s in sides:
            @pl.when(has[axis, s])
            def _(k=k):
                copies[k].wait_send()

    blocks = [(i, k) for i in range(bx) for k in range(by)]

    def row(ref, r):
        return jnp.concatenate([ref[i, k, r : r + 1, :] for i, k in blocks], axis=1)

    samples = traces[...].reshape(nj, ns)
    sample_ids = lax.broadcasted_iota(jnp.int32, (ns, nt), 0).astype(F32).astype(BF)
    quarter = traveltime[...]
    first = (quarter >> 2).astype(F32)
    fraction = (quarter & 3).astype(F32) * 0.25
    first_b, next_b = first.astype(BF), (first + 1.0).astype(BF)
    frac_b, rest_b = fraction.astype(BF), (1.0 - fraction).astype(BF)
    zero = jnp.zeros((), BF)
    for c in range(nc):
        interp = jnp.where(
            sample_ids == first_b[c : c + 1, :],
            rest_b[c : c + 1, :],
            jnp.where(sample_ids == next_b[c : c + 1, :], frac_b[c : c + 1, :], zero),
        )
        taps[c] = jnp.dot(samples, interp, preferred_element_type=F32).astype(BF)

    for b, (i, k) in enumerate(blocks):
        offset_row = geometry[i, k, 2:3, :].astype(F32)
        offset_col = jnp.broadcast_to(offset_row, (tr, tr)).T.astype(BF)
        for r in range(0, tr, 16):
            rows = pl.ds(b * tr + r, 16)
            o = offset_col[r : r + 16, :]
            o = jnp.concatenate([o] * (nt // tr), axis=1)
            at_class = [taps[c, rows, :] for c in range(nc)]
            is_offset = [o == BF(h) for h in range(nh)]
            for d in range(ND):
                value = at_class[d]
                for h in range(1, nh):
                    value = jnp.where(is_offset[h], at_class[d + h], value)
                values[pl.ds(d * nj + b * tr + r, 16), :] = value

    offset = row(geometry, 2)
    trace_weight = jnp.concatenate([weight[i, k : k + 1, :] for i, k in blocks], axis=1).astype(F32)
    scaled = []
    for d in range(ND):
        factor = jnp.zeros((1, nj), F32)
        for h in range(nh):
            factor = jnp.where(offset == h, class_weight[h + d], factor)
        scaled.append((trace_weight * factor).astype(BF).astype(F32))

    point = lax.broadcasted_iota(jnp.int32, (cols, nj), 0)
    point_x = (point // PY).astype(F32).astype(BF)
    point_y = (point % PY).astype(F32).astype(BF)
    mid_x = (row(geometry, 0) - me_x * PX).astype(F32)
    mid_y = (row(geometry, 1) - me_y * PY).astype(F32)
    grid = 136.0
    shift = (DSTEP - 1) / (2 * DSTEP)
    away_x = {
        dx: jnp.abs(point_x - (mid_x - dx * PX).astype(BF)) * BF(1 / DSTEP) for dx in (-1, 0, 1)
    }
    away_y = {
        dy: jnp.abs(point_y - (mid_y - dy * PY).astype(BF)) * BF(1 / DSTEP) - BF(shift)
        for dy in (-1, 0, 1)
    }

    def migrate(tiles):
        depth = classes_at(*tiles[0]) * nj
        for n, (dx, dy) in enumerate(tiles):
            level = (away_x[dx] + away_y[dy]) + BF(grid)
            entry = (dx + 1) * 3 + (dy + 1)
            live = jnp.concatenate(
                [jnp.full((1, tr), aperture[i, k, entry], jnp.int32) for i, k in blocks], axis=1
            ).astype(F32)
            for d in range(classes_at(dx, dy)):
                amplitude[pl.ds(n * cols, cols), pl.ds(d * nj, nj)] = jnp.where(
                    level == BF(grid + d), (scaled[d] * live).astype(BF), zero
                )
        part = jnp.dot(
            amplitude[pl.ds(0, len(tiles) * cols), pl.ds(0, depth)],
            values[pl.ds(0, depth), :],
            preferred_element_type=F32,
        )
        return [part[n * cols : (n + 1) * cols] for n in range(len(tiles))]

    parts = migrate([(-1, -1), (1, -1), (-1, 1), (1, 1)])
    for n in range(4):
        diag_out[n // 2, n % 2] = parts[n].astype(BF)
    pl.semaphore_wait(barrier, sum(there.astype(jnp.int32) for there in has.values()))
    start(diag, "gy")
    parts = migrate([(0, -1), (0, 1)])
    for n in range(2):
        side_out[n] = parts[n].astype(BF)
    start(side, "gy")
    parts = migrate([(-1, 0), (1, 0)])
    arrive(diag, "gy", diag_in)
    for n in range(2):
        x_out[n] = (parts[n] + diag_in[0, n].astype(F32) + diag_in[1, n].astype(F32)).astype(BF)
    start(across, "gx")
    parts = migrate([(0, 0)])
    arrive(side, "gy", side_in)
    total = parts[0] + side_in[0].astype(F32) + side_in[1].astype(F32)
    arrive(across, "gx", x_in)
    image[...] = total + x_in[0].astype(F32) + x_in[1].astype(F32)
    sent(diag, "gy")
    sent(side, "gy")
    sent(across, "gx")


def per_device(n_x, n_y, traces, aperture, geometry, trace_weight, class_weight, traveltime):
    bx, by, tr, ns = traces.shape
    nc, nt = traveltime.shape
    nj = bx * by * tr
    cols = PX * PY
    vmem = pl.BlockSpec(memory_space=pltpu.VMEM)
    smem = pl.BlockSpec(memory_space=pltpu.SMEM)
    image = pl.pallas_call(
        functools.partial(kernel, n_x, n_y),
        out_shape=jax.ShapeDtypeStruct((cols, nt), F32),
        in_specs=[vmem] * 4 + [smem] * 2,
        out_specs=vmem,
        scratch_shapes=[
            pltpu.VMEM((nc, nj, nt), BF),
            pltpu.VMEM((ND * nj, nt), BF),
            pltpu.VMEM((4 * cols, ND * nj), BF),
            pltpu.VMEM((2, 2, cols, nt), BF),
            pltpu.VMEM((2, cols, nt), BF),
            pltpu.VMEM((2, cols, nt), BF),
            pltpu.VMEM((2, 2, cols, nt), BF),
            pltpu.VMEM((2, cols, nt), BF),
            pltpu.VMEM((2, cols, nt), BF),
            pltpu.SemaphoreType.DMA((6,)),
            pltpu.SemaphoreType.DMA((6,)),
        ],
        compiler_params=pltpu.CompilerParams(collective_id=0, has_side_effects=True),
    )(traces, geometry, trace_weight, traveltime, aperture, class_weight)
    return image.reshape(PX, PY, nt)


def solution(mesh):
    return jax.shard_map(
        functools.partial(per_device, mesh.shape["gx"], mesh.shape["gy"]),
        mesh=mesh,
        in_specs=(
            P("gx", "gy", None, None),
            P("gx", "gy", None),
            P("gx", "gy", None, None),
            P("gx", "gy", None),
            P(),
            P(),
        ),
        out_specs=P("gx", "gy", None),
        check_vma=False,
    )
```

```python
import functools

import jax
import jax.numpy as jnp
from jax import lax
from jax.experimental import pallas as pl
from jax.experimental.pallas import tpu as pltpu
from jax.sharding import PartitionSpec as P

PX = 16
PY = 8
DSTEP = 8
MESH = pl.DeviceIdType.MESH
BF = jnp.bfloat16
F32 = jnp.float32

ND = (2 * PX - 1 + 2 * PY - 1) // DSTEP + 1


def classes_at(dx, dy):
    far_x = 2 * PX - 1 if dx else PX - 1
    far_y = 2 * PY - 1 if dy else PY - 1
    return (far_x + far_y) // DSTEP + 1


def kernel(
    n_x, n_y, traces_at, geometry_at, weight_at, traveltime_at, aperture_at, class_weight_at,
    total, from_x, traces, geometry, weight, traveltime, aperture, class_weight,
    interp, taps, values, amplitude, own, y_out, y_in, x_out, x_in,
    load_sem, send_sem, recv_sem,
):
    loads = [
        pltpu.make_async_copy(src, dst, load_sem.at[n])
        for n, (src, dst) in enumerate(
            (
                (traveltime_at, traveltime), (traces_at, traces), (geometry_at, geometry),
                (weight_at, weight), (aperture_at, aperture), (class_weight_at, class_weight),
            )
        )
    ]
    for load in loads:
        load.start()
    bx, by, tr, ns = traces.shape
    nc, nt = traveltime.shape
    nj = bx * by * tr
    cols = PX * PY
    nh = nc - ND + 1
    me_x = lax.axis_index("gx")
    me_y = lax.axis_index("gy")
    turn = 2 * lax.rem(me_x, 2) - 1
    step_x = (turn, -turn)
    step_y = (-1, 1)
    has_x = [jnp.logical_and(me_x + s >= 0, me_x + s < n_x) for s in step_x]
    has_y = [me_y > 0, me_y < n_y - 1]
    barrier = pltpu.get_barrier_semaphore()
    for k in range(2):
        @pl.when(has_x[k])
        def _(k=k):
            pl.semaphore_signal(
                barrier, inc=1, device_id={"gx": me_x + step_x[k]}, device_id_type=MESH
            )

        @pl.when(has_y[k])
        def _(k=k):
            pl.semaphore_signal(
                barrier, inc=1, device_id={"gy": me_y + step_y[k]}, device_id_type=MESH
            )

    def copy(src, dst, number, device):
        return pltpu.make_async_remote_copy(
            src_ref=src, dst_ref=dst,
            send_sem=send_sem.at[number], recv_sem=recv_sem.at[number],
            device_id=device, device_id_type=MESH,
        )

    along_y = [
        [copy(y_out.at[n, k], y_in.at[n, k], 2 * n + k, {"gy": me_y + step_y[k]}) for k in range(2)]
        for n in range(3)
    ]
    along_x = [
        copy(x_out.at[k], x_in.at[k], 6 + k, {"gx": me_x + step_x[k]}) for k in range(2)
    ]

    def when(there, act):
        pl.when(there)(act)

    def send_y(n):
        for k in range(2):
            when(has_y[k], along_y[n][k].start)

    def arrive_y(n):
        for k in range(2):
            when(has_y[1 - k], along_y[n][k].wait_recv)

    for k in range(2):
        @pl.when(jnp.logical_not(has_y[1 - k]))
        def _(k=k):
            for n in range(3):
                y_in[n, k] = jnp.zeros(y_in.shape[2:], BF)

        @pl.when(jnp.logical_not(has_x[k]))
        def _(k=k):
            x_in[k] = jnp.zeros(x_in.shape[1:], BF)

    blocks = [(i, k) for i in range(bx) for k in range(by)]

    def row(ref, r):
        return jnp.concatenate([ref[i, r, k : k + 1, :] for i, k in blocks], axis=1)

    sample_ids = lax.broadcasted_iota(jnp.int32, (ns, nt), 0).astype(F32).astype(BF)
    zero = jnp.zeros((), BF)
    loads[0].wait()
    quarter = traveltime[...]
    first = (quarter >> 2).astype(F32)
    fraction = (quarter & 3).astype(F32) * 0.25
    first_b, next_b = first.astype(BF), (first + 1.0).astype(BF)
    frac_b, rest_b = fraction.astype(BF), (1.0 - fraction).astype(BF)
    for c in range(nc):
        interp[c] = jnp.where(
            sample_ids == first_b[c : c + 1, :],
            rest_b[c : c + 1, :],
            jnp.where(sample_ids == next_b[c : c + 1, :], frac_b[c : c + 1, :], zero),
        )

    for load in loads[1:]:
        load.wait()
    samples = traces[...].reshape(nj, ns)
    for c in range(nc):
        taps[c] = jnp.dot(samples, interp[c], preferred_element_type=F32).astype(BF)

    for b, (i, k) in enumerate(blocks):
        offset_row = geometry[i, 2, k : k + 1, :].astype(F32)
        offset_col = jnp.broadcast_to(offset_row, (tr, tr)).T.astype(BF)
        for r in range(0, tr, 16):
            rows = pl.ds(b * tr + r, 16)
            o = offset_col[r : r + 16, :]
            value = at_class = [
                [taps[c, rows, pl.ds(t, tr)] for t in range(0, nt, tr)] for c in range(nc)
            ]
            is_last = o == BF(nh - 1)
            bit = 1
            while 2 * bit < nh - 1:
                bit *= 2
            while bit:
                digit = o >= BF(bit)
                o = jnp.where(digit, o - BF(bit), o)
                value = [
                    [jnp.where(digit, high, low) for high, low in zip(value[c + bit], value[c])]
                    for c in range(ND + bit - 1)
                ]
                bit //= 2
            value[ND - 1] = [
                jnp.where(is_last, last, v) for last, v in zip(at_class[nc - 1], value[ND - 1])
            ]
            for d in range(ND):
                for n, v in enumerate(value[d]):
                    values[pl.ds(d * nj + b * tr + r, 16), pl.ds(n * tr, tr)] = v

    offset = row(geometry, 2)
    trace_weight = jnp.concatenate([weight[i, k : k + 1, :] for i, k in blocks], axis=1).astype(F32)
    scaled = []
    for d in range(ND):
        factor = jnp.zeros((1, nj), F32)
        for h in range(nh):
            factor = jnp.where(offset == h, class_weight[h + d], factor)
        scaled.append((trace_weight * factor).astype(BF).astype(F32))

    point = lax.broadcasted_iota(jnp.int32, (cols, nj), 0)
    point_x = (point // PY).astype(F32).astype(BF)
    point_y = (point % PY).astype(F32).astype(BF)
    mid_x = row(geometry, 0) - me_x * PX
    mid_y = row(geometry, 1) - me_y * PY
    grid = 136.0
    shift = (DSTEP - 1) / (2 * DSTEP)
    away_x = {
        dx: jnp.abs(point_x - (mid_x - at * PX).astype(F32).astype(BF)) * BF(1 / DSTEP)
        for dx, at in ((0, 0), (1, turn), (-1, -turn))
    }
    away_y = {
        dy: jnp.abs(point_y - (mid_y - dy * PY).astype(F32).astype(BF)) * BF(1 / DSTEP) - BF(shift)
        for dy in (-1, 0, 1)
    }

    def migrate(tiles):
        depth = classes_at(*tiles[0]) * nj
        for n, (dx, dy) in enumerate(tiles):
            level = (away_x[dx] + away_y[dy]) + BF(grid)
            entry = (dx * turn + 1) * 3 + (dy + 1)
            live = jnp.concatenate(
                [jnp.full((1, tr), aperture[i, k, entry], jnp.int32) for i, k in blocks], axis=1
            ).astype(F32)
            for d in range(classes_at(dx, dy)):
                amplitude[pl.ds(n * cols, cols), pl.ds(d * nj, nj)] = jnp.where(
                    level == BF(grid + d), (scaled[d] * live).astype(BF), zero
                )
        part = jnp.dot(
            amplitude[pl.ds(0, len(tiles) * cols), pl.ds(0, depth)],
            values[pl.ds(0, depth), :],
            preferred_element_type=F32,
        )
        return [part[n * cols : (n + 1) * cols] for n in range(len(tiles))]

    for n, dx in enumerate((1, -1, 0)):
        for k, part in enumerate(migrate([(dx, -1), (dx, 1)])):
            y_out[n, k] = part.astype(BF)
        if n == 0:
            there = [t.astype(jnp.int32) for t in has_x + has_y]
            pl.semaphore_wait(barrier, sum(there))
        send_y(n)
    for k, part in enumerate(migrate([(1, 0), (-1, 0)])):
        own[k] = part
    own[2] = migrate([(0, 0)])[0]

    def summed(n):
        arrive_y(n)
        return own[n] + y_in[n, 0].astype(F32) + y_in[n, 1].astype(F32)

    for k in range(2):
        x_out[k] = summed(k).astype(BF)
        when(has_x[k], along_x[k].start)
    total[...] = summed(2)
    for k in range(2):
        when(has_x[k], along_x[k].wait_recv)
        from_x[k] = x_in[k]
    for k in range(2):
        for n in range(3):
            when(has_y[k], along_y[n][k].wait_send)
        when(has_x[k], along_x[k].wait_send)


def per_device(n_x, n_y, traces, aperture, geometry, trace_weight, class_weight, traveltime):
    bx, by, tr, ns = traces.shape
    nc, nt = traveltime.shape
    nj = bx * by * tr
    cols = PX * PY
    geometry = jnp.transpose(geometry, (0, 2, 1, 3))
    vmem = pl.BlockSpec(memory_space=pltpu.VMEM)
    total, from_x = pl.pallas_call(
        functools.partial(kernel, n_x, n_y),
        out_shape=(pltpu.VMEM((cols, nt), F32), pltpu.VMEM((2, cols, nt), BF)),
        in_specs=[pl.BlockSpec(memory_space=pltpu.HBM)] * 6,
        out_specs=(vmem, vmem),
        scratch_shapes=[
            pltpu.VMEM(traces.shape, traces.dtype),
            pltpu.VMEM(geometry.shape, geometry.dtype),
            pltpu.VMEM(trace_weight.shape, trace_weight.dtype),
            pltpu.VMEM(traveltime.shape, traveltime.dtype),
            pltpu.SMEM(aperture.shape, aperture.dtype),
            pltpu.SMEM(class_weight.shape, class_weight.dtype),
            pltpu.VMEM((nc, ns, nt), BF),
            pltpu.VMEM((nc, nj, nt), BF),
            pltpu.VMEM((ND * nj, nt), BF),
            pltpu.VMEM((2 * cols, ND * nj), BF),
            pltpu.VMEM((3, cols, nt), F32),
            pltpu.VMEM((3, 2, cols, nt), BF),
            pltpu.VMEM((3, 2, cols, nt), BF),
            pltpu.VMEM((2, cols, nt), BF),
            pltpu.VMEM((2, cols, nt), BF),
            pltpu.SemaphoreType.DMA((6,)),
            pltpu.SemaphoreType.DMA((8,)),
            pltpu.SemaphoreType.DMA((8,)),
        ],
        compiler_params=pltpu.CompilerParams(collective_id=0, has_side_effects=True),
    )(traces, geometry, trace_weight, traveltime, aperture, class_weight)
    image = total + from_x[0].astype(F32) + from_x[1].astype(F32)
    return image.reshape(PX, PY, nt)


def solution(mesh):
    return jax.shard_map(
        functools.partial(per_device, mesh.shape["gx"], mesh.shape["gy"]),
        mesh=mesh,
        in_specs=(
            P("gx", "gy", None, None),
            P("gx", "gy", None),
            P("gx", "gy", None, None),
            P("gx", "gy", None),
            P(),
            P(),
        ),
        out_specs=P("gx", "gy", None),
        check_vma=False,
    )
```

```python
import functools

import jax
import jax.numpy as jnp
from jax import lax
from jax.experimental import pallas as pl
from jax.experimental.pallas import tpu as pltpu
from jax.sharding import PartitionSpec as P

PX = 16
PY = 8
DSTEP = 8
MESH = pl.DeviceIdType.MESH
BF = jnp.bfloat16
F32 = jnp.float32

ND = (2 * PX - 1 + 2 * PY - 1) // DSTEP + 1


def classes_at(dx, dy):
    far_x = 2 * PX - 1 if dx else PX - 1
    far_y = 2 * PY - 1 if dy else PY - 1
    return (far_x + far_y) // DSTEP + 1


def kernel(
    n_x, n_y, traces_at, geometry_at, weight_at, traveltime_at, aperture_at, class_weight_at,
    total, from_x, traces, geometry, weight, traveltime, aperture, class_weight,
    interp, taps, values, amplitude, own, y_out, y_in, x_out, x_in,
    load_sem, send_sem, recv_sem,
):
    loads = [
        pltpu.make_async_copy(src, dst, load_sem.at[n])
        for n, (src, dst) in enumerate(
            (
                (traveltime_at, traveltime), (traces_at, traces), (geometry_at, geometry),
                (weight_at, weight), (aperture_at, aperture), (class_weight_at, class_weight),
            )
        )
    ]
    for load in loads:
        load.start()
    bx, by, tr, ns = traces.shape
    nc, nt = traveltime.shape
    nj = bx * by * tr
    cols = PX * PY
    nh = nc - ND + 1
    me_x = lax.axis_index("gx")
    me_y = lax.axis_index("gy")
    turn = 2 * lax.rem(me_x, 2) - 1
    step_x = (turn, -turn)
    step_y = (-1, 1)
    has_x = [jnp.logical_and(me_x + s >= 0, me_x + s < n_x) for s in step_x]
    has_y = [me_y > 0, me_y < n_y - 1]
    barrier = pltpu.get_barrier_semaphore()
    for k in range(2):
        @pl.when(has_x[k])
        def _(k=k):
            pl.semaphore_signal(
                barrier, inc=1, device_id={"gx": me_x + step_x[k]}, device_id_type=MESH
            )

        @pl.when(has_y[k])
        def _(k=k):
            pl.semaphore_signal(
                barrier, inc=1, device_id={"gy": me_y + step_y[k]}, device_id_type=MESH
            )

    def copy(src, dst, number, device):
        return pltpu.make_async_remote_copy(
            src_ref=src, dst_ref=dst,
            send_sem=send_sem.at[number], recv_sem=recv_sem.at[number],
            device_id=device, device_id_type=MESH,
        )

    half = cols // 2
    cuts = [pl.ds(m * half, half) for m in range(2)]
    along_y = [
        [
            [
                copy(
                    y_out.at[n, k, cut], y_in.at[n, k, cut], 4 * n + 2 * m + k,
                    {"gy": me_y + step_y[k]},
                )
                for k in range(2)
            ]
            for m, cut in enumerate(cuts)
        ]
        for n in range(3)
    ]
    along_x = [
        [
            copy(
                x_out.at[k, cut], x_in.at[k, cut], 12 + 2 * k + m,
                {"gx": me_x + step_x[k]},
            )
            for m, cut in enumerate(cuts)
        ]
        for k in range(2)
    ]

    def when(there, act):
        pl.when(there)(act)

    def send_y(n):
        for k in range(2):
            @pl.when(has_y[k])
            def _(k=k):
                for m in range(2):
                    along_y[n][m][k].start()

    def arrive_y(n, m):
        for k in range(2):
            when(has_y[1 - k], along_y[n][m][k].wait_recv)

    for k in range(2):
        @pl.when(jnp.logical_not(has_y[1 - k]))
        def _(k=k):
            for n in range(3):
                y_in[n, k] = jnp.zeros(y_in.shape[2:], BF)

        @pl.when(jnp.logical_not(has_x[k]))
        def _(k=k):
            x_in[k] = jnp.zeros(x_in.shape[1:], BF)

    blocks = [(i, k) for i in range(bx) for k in range(by)]

    def row(ref, r):
        return jnp.concatenate([ref[i, r, k : k + 1, :] for i, k in blocks], axis=1)

    sample_ids = lax.broadcasted_iota(jnp.int32, (ns, nt), 0).astype(F32).astype(BF)
    zero = jnp.zeros((), BF)
    loads[0].wait()
    quarter = traveltime[...]
    first = (quarter >> 2).astype(F32)
    fraction = (quarter & 3).astype(F32) * 0.25
    first_b, next_b = first.astype(BF), (first + 1.0).astype(BF)
    frac_b, rest_b = fraction.astype(BF), (1.0 - fraction).astype(BF)
    for c in range(nc):
        interp[c] = jnp.where(
            sample_ids == first_b[c : c + 1, :],
            rest_b[c : c + 1, :],
            jnp.where(sample_ids == next_b[c : c + 1, :], frac_b[c : c + 1, :], zero),
        )

    for load in loads[2:]:
        load.wait()
    offset = row(geometry, 2)
    trace_weight = jnp.concatenate([weight[i, k : k + 1, :] for i, k in blocks], axis=1).astype(F32)
    scaled = []
    for d in range(ND):
        factor = jnp.zeros((1, nj), F32)
        for h in range(nh):
            factor = jnp.where(offset == h, class_weight[h + d], factor)
        scaled.append((trace_weight * factor).astype(BF).astype(F32))

    point = lax.broadcasted_iota(jnp.int32, (cols, nj), 0)
    point_x = (point // PY).astype(F32).astype(BF)
    point_y = (point % PY).astype(F32).astype(BF)
    mid_x = row(geometry, 0) - me_x * PX
    mid_y = row(geometry, 1) - me_y * PY
    grid = 136.0
    shift = (DSTEP - 1) / (2 * DSTEP)
    away_x = {
        dx: jnp.abs(point_x - (mid_x - at * PX).astype(F32).astype(BF)) * BF(1 / DSTEP)
        for dx, at in ((0, 0), (1, turn), (-1, -turn))
    }
    away_y = {
        dy: jnp.abs(point_y - (mid_y - dy * PY).astype(F32).astype(BF)) * BF(1 / DSTEP) - BF(shift)
        for dy in (-1, 0, 1)
    }

    def weigh(tiles, top):
        for n, (dx, dy) in enumerate(tiles):
            level = (away_x[dx] + away_y[dy]) + BF(grid)
            entry = (dx * turn + 1) * 3 + (dy + 1)
            live = jnp.concatenate(
                [jnp.full((1, tr), aperture[i, k, entry], jnp.int32) for i, k in blocks], axis=1
            ).astype(F32)
            for d in range(classes_at(dx, dy)):
                amplitude[pl.ds((top + n) * cols, cols), pl.ds(d * nj, nj)] = jnp.where(
                    level == BF(grid + d), (scaled[d] * live).astype(BF), zero
                )

    def migrate(tiles, top):
        depth = classes_at(*tiles[0]) * nj
        part = jnp.dot(
            amplitude[pl.ds(top * cols, len(tiles) * cols), pl.ds(0, depth)],
            values[pl.ds(0, depth), :],
            preferred_element_type=F32,
        )
        return [part[n * cols : (n + 1) * cols] for n in range(len(tiles))]

    aside = [[(dx, -1), (dx, 1)] for dx in (1, -1, 0)]
    weigh(aside[0], 0)

    loads[1].wait()
    rows_at = nj // 2
    for start in range(0, nj, rows_at):
        samples = traces[...].reshape(nj, ns)[start : start + rows_at]
        for c in range(nc):
            taps[c, pl.ds(start, rows_at), :] = jnp.dot(
                samples, interp[c], preferred_element_type=F32
            ).astype(BF)

    for b, (i, k) in enumerate(blocks):
        offset_row = geometry[i, 2, k : k + 1, :].astype(F32)
        offset_col = jnp.broadcast_to(offset_row, (tr, tr)).T.astype(BF)
        for r in range(0, tr, 16):
            rows = pl.ds(b * tr + r, 16)
            o = offset_col[r : r + 16, :]
            value = at_class = [
                [taps[c, rows, pl.ds(t, tr)] for t in range(0, nt, tr)] for c in range(nc)
            ]
            is_last = o == BF(nh - 1)
            bit = 1
            while 2 * bit < nh - 1:
                bit *= 2
            while bit:
                digit = o >= BF(bit)
                o = jnp.where(digit, o - BF(bit), o)
                value = [
                    [jnp.where(digit, high, low) for high, low in zip(value[c + bit], value[c])]
                    for c in range(ND + bit - 1)
                ]
                bit //= 2
            value[ND - 1] = [
                jnp.where(is_last, last, v) for last, v in zip(at_class[nc - 1], value[ND - 1])
            ]
            for d in range(ND):
                for n, v in enumerate(value[d]):
                    values[pl.ds(d * nj + b * tr + r, 16), pl.ds(n * tr, tr)] = v

    for n, tiles in enumerate(aside):
        if n:
            weigh(tiles, 2 * n)
        for k, part in enumerate(migrate(tiles, 2 * n)):
            y_out[n, k] = part.astype(BF)
        if n == 0:
            there = [t.astype(jnp.int32) for t in has_x + has_y]
            pl.semaphore_wait(barrier, sum(there))
        send_y(n)
    along = [(1, 0), (-1, 0)]
    weigh(along, 6)
    weigh([(0, 0)], 8)
    for k, part in enumerate(migrate(along, 6)):
        own[k] = part
    own[2] = migrate([(0, 0)], 8)[0]

    def summed(n, m):
        cut = cuts[m]
        arrive_y(n, m)
        return own[n, cut] + y_in[n, 0, cut].astype(F32) + y_in[n, 1, cut].astype(F32)

    for k in range(2):
        for m, cut in enumerate(cuts):
            x_out[k, cut] = summed(k, m).astype(BF)
            when(has_x[k], along_x[k][m].start)
    for m, cut in enumerate(cuts):
        total[cut] = summed(2, m)
    for k in range(2):
        for m, cut in enumerate(cuts):
            when(has_x[k], along_x[k][m].wait_recv)
            from_x[k, cut] = x_in[k, cut]
    for k in range(2):
        @pl.when(has_y[k])
        def _(k=k):
            for n in range(3):
                for m in range(2):
                    along_y[n][m][k].wait_send()

        @pl.when(has_x[k])
        def _(k=k):
            for m in range(2):
                along_x[k][m].wait_send()


def per_device(n_x, n_y, traces, aperture, geometry, trace_weight, class_weight, traveltime):
    bx, by, tr, ns = traces.shape
    nc, nt = traveltime.shape
    nj = bx * by * tr
    cols = PX * PY
    geometry = jnp.transpose(geometry, (0, 2, 1, 3))
    vmem = pl.BlockSpec(memory_space=pltpu.VMEM)
    total, from_x = pl.pallas_call(
        functools.partial(kernel, n_x, n_y),
        out_shape=(pltpu.VMEM((cols, nt), F32), pltpu.VMEM((2, cols, nt), BF)),
        in_specs=[pl.BlockSpec(memory_space=pltpu.HBM)] * 6,
        out_specs=(vmem, vmem),
        scratch_shapes=[
            pltpu.VMEM(traces.shape, traces.dtype),
            pltpu.VMEM(geometry.shape, geometry.dtype),
            pltpu.VMEM(trace_weight.shape, trace_weight.dtype),
            pltpu.VMEM(traveltime.shape, traveltime.dtype),
            pltpu.SMEM(aperture.shape, aperture.dtype),
            pltpu.SMEM(class_weight.shape, class_weight.dtype),
            pltpu.VMEM((nc, ns, nt), BF),
            pltpu.VMEM((nc, nj, nt), BF),
            pltpu.VMEM((ND * nj, nt), BF),
            pltpu.VMEM((9 * cols, ND * nj), BF),
            pltpu.VMEM((3, cols, nt), F32),
            pltpu.VMEM((3, 2, cols, nt), BF),
            pltpu.VMEM((3, 2, cols, nt), BF),
            pltpu.VMEM((2, cols, nt), BF),
            pltpu.VMEM((2, cols, nt), BF),
            pltpu.SemaphoreType.DMA((6,)),
            pltpu.SemaphoreType.DMA((16,)),
            pltpu.SemaphoreType.DMA((16,)),
        ],
        compiler_params=pltpu.CompilerParams(collective_id=0, has_side_effects=True),
    )(traces, geometry, trace_weight, traveltime, aperture, class_weight)
    image = total + from_x[0].astype(F32) + from_x[1].astype(F32)
    return image.reshape(PX, PY, nt)


def solution(mesh):
    return jax.shard_map(
        functools.partial(per_device, mesh.shape["gx"], mesh.shape["gy"]),
        mesh=mesh,
        in_specs=(
            P("gx", "gy", None, None),
            P("gx", "gy", None),
            P("gx", "gy", None, None),
            P("gx", "gy", None),
            P(),
            P(),
        ),
        out_specs=P("gx", "gy", None),
        check_vma=False,
    )
```

```python
import functools

import jax
import jax.numpy as jnp
from jax import lax
from jax.experimental import pallas as pl
from jax.experimental.pallas import tpu as pltpu
from jax.sharding import PartitionSpec as P

PX = 16
PY = 8
DSTEP = 8
MESH = pl.DeviceIdType.MESH
BF = jnp.bfloat16
F32 = jnp.float32

ND = (2 * PX - 1 + 2 * PY - 1) // DSTEP + 1


def classes_at(dx, dy):
    far_x = 2 * PX - 1 if dx else PX - 1
    far_y = 2 * PY - 1 if dy else PY - 1
    return (far_x + far_y) // DSTEP + 1


def kernel(
    n_x, n_y, traces_at, geometry_at, weight_at, traveltime_at, aperture_at, class_weight_at,
    total, from_x, traces, geometry, weight, traveltime, aperture, class_weight,
    interp, taps, values, amplitude, own, y_out, y_in, x_out, x_in,
    load_sem, send_sem, recv_sem,
):
    loads = [
        pltpu.make_async_copy(src, dst, load_sem.at[n])
        for n, (src, dst) in enumerate(
            (
                (traveltime_at, traveltime), (traces_at, traces), (geometry_at, geometry),
                (weight_at, weight), (aperture_at, aperture), (class_weight_at, class_weight),
            )
        )
    ]
    for load in loads:
        load.start()
    bx, by, tr, ns = traces.shape
    nc, nt = traveltime.shape
    nj = bx * by * tr
    cols = PX * PY
    nh = nc - ND + 1
    me_x = lax.axis_index("gx")
    me_y = lax.axis_index("gy")
    turn = 2 * lax.rem(me_x, 2) - 1
    step_x = (turn, -turn)
    step_y = (-1, 1)
    has_x = [jnp.logical_and(me_x + s >= 0, me_x + s < n_x) for s in step_x]
    has_y = [me_y > 0, me_y < n_y - 1]
    barrier = pltpu.get_barrier_semaphore()
    for k in range(2):
        @pl.when(has_x[k])
        def _(k=k):
            pl.semaphore_signal(
                barrier, inc=1, device_id={"gx": me_x + step_x[k]}, device_id_type=MESH
            )

        @pl.when(has_y[k])
        def _(k=k):
            pl.semaphore_signal(
                barrier, inc=1, device_id={"gy": me_y + step_y[k]}, device_id_type=MESH
            )

    def copy(src, dst, number, device):
        return pltpu.make_async_remote_copy(
            src_ref=src, dst_ref=dst,
            send_sem=send_sem.at[number], recv_sem=recv_sem.at[number],
            device_id=device, device_id_type=MESH,
        )

    half = cols // 2
    cuts = [pl.ds(m * half, half) for m in range(2)]
    along_y = [
        [
            [
                copy(
                    y_out.at[n, k, cut], y_in.at[n, k, cut], 4 * n + 2 * m + k,
                    {"gy": me_y + step_y[k]},
                )
                for k in range(2)
            ]
            for m, cut in enumerate(cuts)
        ]
        for n in range(3)
    ]
    along_x = [
        [
            copy(
                x_out.at[k, cut], x_in.at[k, cut], 12 + 2 * k + m,
                {"gx": me_x + step_x[k]},
            )
            for m, cut in enumerate(cuts)
        ]
        for k in range(2)
    ]

    def when(there, act):
        pl.when(there)(act)

    def send_y(n):
        for k in range(2):
            @pl.when(has_y[k])
            def _(k=k):
                for m in range(2):
                    along_y[n][m][k].start()

    def arrive_y(n, m):
        for k in range(2):
            when(has_y[1 - k], along_y[n][m][k].wait_recv)

    for k in range(2):
        @pl.when(jnp.logical_not(has_y[1 - k]))
        def _(k=k):
            for n in range(3):
                y_in[n, k] = jnp.zeros(y_in.shape[2:], BF)

        @pl.when(jnp.logical_not(has_x[k]))
        def _(k=k):
            x_in[k] = jnp.zeros(x_in.shape[1:], BF)

    blocks = [(i, k) for i in range(bx) for k in range(by)]

    def row(ref, r):
        return jnp.concatenate([ref[i, r, k : k + 1, :] for i, k in blocks], axis=1)

    sample_ids = lax.broadcasted_iota(jnp.int32, (ns, nt), 0).astype(F32).astype(BF)
    zero = jnp.zeros((), BF)
    loads[0].wait()
    quarter = traveltime[...]
    first = (quarter >> 2).astype(F32)
    fraction = (quarter & 3).astype(F32) * 0.25
    first_b, next_b = first.astype(BF), (first + 1.0).astype(BF)
    frac_b, rest_b = fraction.astype(BF), (1.0 - fraction).astype(BF)
    for c in range(nc):
        interp[c] = jnp.where(
            sample_ids == first_b[c : c + 1, :],
            rest_b[c : c + 1, :],
            jnp.where(sample_ids == next_b[c : c + 1, :], frac_b[c : c + 1, :], zero),
        )

    for load in loads[1:]:
        load.wait()
    samples = traces[...].reshape(nj, ns)
    for c in range(nc):
        taps[c] = jnp.dot(samples, interp[c], preferred_element_type=F32).astype(BF)

    for b, (i, k) in enumerate(blocks):
        offset_row = geometry[i, 2, k : k + 1, :].astype(F32)
        offset_col = jnp.broadcast_to(offset_row, (tr, tr)).T.astype(BF)
        for r in range(0, tr, 16):
            rows = pl.ds(b * tr + r, 16)
            o = offset_col[r : r + 16, :]
            value = at_class = [
                [taps[c, rows, pl.ds(t, tr)] for t in range(0, nt, tr)] for c in range(nc)
            ]
            is_last = o == BF(nh - 1)
            bit = 1
            while 2 * bit < nh - 1:
                bit *= 2
            while bit:
                digit = o >= BF(bit)
                o = jnp.where(digit, o - BF(bit), o)
                value = [
                    [jnp.where(digit, high, low) for high, low in zip(value[c + bit], value[c])]
                    for c in range(ND + bit - 1)
                ]
                bit //= 2
            value[ND - 1] = [
                jnp.where(is_last, last, v) for last, v in zip(at_class[nc - 1], value[ND - 1])
            ]
            for d in range(ND):
                for n, v in enumerate(value[d]):
                    values[pl.ds(d * nj + b * tr + r, 16), pl.ds(n * tr, tr)] = v

    offset = row(geometry, 2)
    trace_weight = jnp.concatenate([weight[i, k : k + 1, :] for i, k in blocks], axis=1).astype(F32)
    scaled = []
    for d in range(ND):
        factor = jnp.zeros((1, nj), F32)
        for h in range(nh):
            factor = jnp.where(offset == h, class_weight[h + d], factor)
        scaled.append((trace_weight * factor).astype(BF).astype(F32))

    point = lax.broadcasted_iota(jnp.int32, (cols, nj), 0)
    point_x = (point // PY).astype(F32).astype(BF)
    point_y = (point % PY).astype(F32).astype(BF)
    mid_x = row(geometry, 0) - me_x * PX
    mid_y = row(geometry, 1) - me_y * PY
    grid = 136.0
    shift = (DSTEP - 1) / (2 * DSTEP)
    away_x = {
        dx: jnp.abs(point_x - (mid_x - at * PX).astype(F32).astype(BF)) * BF(1 / DSTEP)
        for dx, at in ((0, 0), (1, turn), (-1, -turn))
    }
    away_y = {
        dy: jnp.abs(point_y - (mid_y - dy * PY).astype(F32).astype(BF)) * BF(1 / DSTEP) - BF(shift)
        for dy in (-1, 0, 1)
    }

    def migrate(tiles):
        depth = classes_at(*tiles[0]) * nj
        for n, (dx, dy) in enumerate(tiles):
            level = (away_x[dx] + away_y[dy]) + BF(grid)
            entry = (dx * turn + 1) * 3 + (dy + 1)
            live = jnp.concatenate(
                [jnp.full((1, tr), aperture[i, k, entry], jnp.int32) for i, k in blocks], axis=1
            ).astype(F32)
            for d in range(classes_at(dx, dy)):
                amplitude[pl.ds(n * cols, cols), pl.ds(d * nj, nj)] = jnp.where(
                    level == BF(grid + d), (scaled[d] * live).astype(BF), zero
                )
        part = jnp.dot(
            amplitude[pl.ds(0, len(tiles) * cols), pl.ds(0, depth)],
            values[pl.ds(0, depth), :],
            preferred_element_type=F32,
        )
        return [part[n * cols : (n + 1) * cols] for n in range(len(tiles))]

    for n, dx in enumerate((1, -1, 0)):
        for k, part in enumerate(migrate([(dx, -1), (dx, 1)])):
            y_out[n, k] = part.astype(BF)
        if n == 0:
            there = [t.astype(jnp.int32) for t in has_x + has_y]
            pl.semaphore_wait(barrier, sum(there))
        send_y(n)
    for k, part in enumerate(migrate([(1, 0), (-1, 0)])):
        own[k] = part
    own[2] = migrate([(0, 0)])[0]

    def summed(n, m):
        cut = cuts[m]
        arrive_y(n, m)
        return own[n, cut] + y_in[n, 0, cut].astype(F32) + y_in[n, 1, cut].astype(F32)

    for k in range(2):
        for m, cut in enumerate(cuts):
            x_out[k, cut] = summed(k, m).astype(BF)
            when(has_x[k], along_x[k][m].start)
    for m, cut in enumerate(cuts):
        total[cut] = summed(2, m)
    for k in range(2):
        for m, cut in enumerate(cuts):
            when(has_x[k], along_x[k][m].wait_recv)
            from_x[k, cut] = x_in[k, cut]
    for k in range(2):
        @pl.when(has_y[k])
        def _(k=k):
            for n in range(3):
                for m in range(2):
                    along_y[n][m][k].wait_send()

        @pl.when(has_x[k])
        def _(k=k):
            for m in range(2):
                along_x[k][m].wait_send()


def per_device(n_x, n_y, traces, aperture, geometry, trace_weight, class_weight, traveltime):
    bx, by, tr, ns = traces.shape
    nc, nt = traveltime.shape
    nj = bx * by * tr
    cols = PX * PY
    geometry = jnp.transpose(geometry, (0, 2, 1, 3))
    vmem = pl.BlockSpec(memory_space=pltpu.VMEM)
    total, from_x = pl.pallas_call(
        functools.partial(kernel, n_x, n_y),
        out_shape=(pltpu.VMEM((cols, nt), F32), pltpu.VMEM((2, cols, nt), BF)),
        in_specs=[pl.BlockSpec(memory_space=pltpu.HBM)] * 6,
        out_specs=(vmem, vmem),
        scratch_shapes=[
            pltpu.VMEM(traces.shape, traces.dtype),
            pltpu.VMEM(geometry.shape, geometry.dtype),
            pltpu.VMEM(trace_weight.shape, trace_weight.dtype),
            pltpu.VMEM(traveltime.shape, traveltime.dtype),
            pltpu.SMEM(aperture.shape, aperture.dtype),
            pltpu.SMEM(class_weight.shape, class_weight.dtype),
            pltpu.VMEM((nc, ns, nt), BF),
            pltpu.VMEM((nc, nj, nt), BF),
            pltpu.VMEM((ND * nj, nt), BF),
            pltpu.VMEM((2 * cols, ND * nj), BF),
            pltpu.VMEM((3, cols, nt), F32),
            pltpu.VMEM((3, 2, cols, nt), BF),
            pltpu.VMEM((3, 2, cols, nt), BF),
            pltpu.VMEM((2, cols, nt), BF),
            pltpu.VMEM((2, cols, nt), BF),
            pltpu.SemaphoreType.DMA((6,)),
            pltpu.SemaphoreType.DMA((16,)),
            pltpu.SemaphoreType.DMA((16,)),
        ],
        compiler_params=pltpu.CompilerParams(collective_id=0, has_side_effects=True),
    )(traces, geometry, trace_weight, traveltime, aperture, class_weight)
    image = total + from_x[0].astype(F32) + from_x[1].astype(F32)
    return image.reshape(PX, PY, nt)


def solution(mesh):
    return jax.shard_map(
        functools.partial(per_device, mesh.shape["gx"], mesh.shape["gy"]),
        mesh=mesh,
        in_specs=(
            P("gx", "gy", None, None),
            P("gx", "gy", None),
            P("gx", "gy", None, None),
            P("gx", "gy", None),
            P(),
            P(),
        ),
        out_specs=P("gx", "gy", None),
        check_vma=False,
    )
```
